32 devices in a mesh: freq: 2 (over core), row: 4 (over y, x), col: 4 (over z).
Axes of the slice: x: 2, y: 2, z: 4, core: 2. Of those that a mesh axis runs over, the one named last changes fastest.
Arguments:
- coupling: bfloat16 [6144, 6144], P('row', 'col'), may hold values from -0.15625 to 0.15625
- freq_weight: float32 [12288], P(('freq', 'row')), parts along dimension 0, may hold values from 0.05 to 2
Outputs:
- response: float32 [12288, 6144], P(('freq', 'row'), 'col'), parts along dimension 0
The draws below stay inside these ranges and needn't reach their ends.
There are 2 independent parts, one for each index of `freq`. The reference program is written for one: setup_inputs(seed, part) draws one part's arguments, and reference() takes and returns one part's arrays. A program takes and returns all parts, laid end to end along the dimension named above; an argument that names none is the same for every part. Nothing has to cross between parts.
All inputs are finite; a program needn't handle non-finite values.
Results may differ from the reference program's by a relative error of at most 0.0021.
Values may be sent and summed in bfloat16 or wider, within the bound.
A program may use at most 128 MiB of HBM per device.

```python
import jax
import jax.numpy as jnp
from jax import lax

NAUX = 6144
NV = 6144


def draw_freq_weight(key, part):
    key_level = jax.random.fold_in(key, 11)
    key_floor = jax.random.fold_in(key, 23)
    level = jax.random.uniform(key_level, (NV,), jnp.float32)
    values = 0.05 * jnp.exp(level * jnp.log(40.0))
    at_floor = jax.random.uniform(key_floor, (NV,), jnp.float32) < 0.1
    values = jnp.where(at_floor, jnp.float32(0.05), values)
    return jnp.clip(values, 0.05, 2.0).astype(jnp.float32)


def block_levels(own_key, extent, shards, least, high):
    loudness, own = 1.0, jax.random.fold_in(own_key, 6)
    for position, parts in shards:
        draws = jnp.exp(jax.random.uniform(jax.random.fold_in(own, position), (parts,), jnp.float32, least / len(shards), high / len(shards)))
        loudness = loudness * jnp.repeat(draws, extent[position] // parts).reshape([-1 if axis == position else 1 for axis in range(len(extent))])
    return loudness


def centred(key, shape, spread, most, split=(), dtype=jnp.bfloat16):
    array = spread * jax.random.normal(key, shape, jnp.float32)
    if split:
        array = array * block_levels(key, shape, split, -0.22, 0.18)
    return jnp.clip(array, -most, most).astype(dtype)


def setup_inputs(seed: int = 0, part: int = 0) -> dict:
    splits = jax.random.split(jax.random.key(seed), 3)
    own_keys = jax.random.split(jax.random.fold_in(splits[2], part), 3)
    return {
        "coupling": centred(splits[0], (NV, NAUX), (NV // 4) ** -0.5, 0.15625, ((0, 4), (1, 4))),
        "freq_weight": draw_freq_weight(jax.random.fold_in(jax.random.fold_in(splits[2], part), 71), part),
    }


def reference(coupling, freq_weight):
    weighted = (coupling.astype(jnp.float32) * freq_weight[:, None]).astype(jnp.bfloat16)
    return jnp.dot(weighted.astype(jnp.float32).T, coupling.astype(jnp.float32),
                   precision=lax.Precision.HIGHEST, preferred_element_type=jnp.float32)
```

```python
import functools

import jax
import jax.numpy as jnp
from jax import lax
from jax.experimental import pallas as pl
from jax.experimental.pallas import tpu as pltpu
from jax.sharding import PartitionSpec as P

MESH = pl.DeviceIdType.MESH
SIDE = 2


def kernel(cols_n, K, CH, c_ref, w_ref, o_ref, X, T, W, acc, load, wsend, wrecv, zr, zup, zdn, tl, nr, nx, ny, nrl,
           ms, mr, ds, dr, osem):
    f = lax.axis_index("freq")
    r = lax.axis_index("row")
    z = lax.axis_index("col")
    rows_n = SIDE * SIDE
    H = CH // 2
    other = 1 - f
    xn, yn, dg = r ^ 1, r ^ 2, r ^ 3
    plane = (xn, yn, dg)
    mi = jnp.where(r == z, 0, 1)
    width = c_ref.shape[1]

    def rows_of(k, core):
        return pl.ds(pl.multiple_of(k * CH + core * H, H), H)

    def trow(k):
        return pl.ds(pl.multiple_of(k * H, H), H)

    def rcopy(src, dst, s, d, dev):
        return pltpu.make_async_remote_copy(src_ref=src, dst_ref=dst, send_sem=s, recv_sem=d, device_id=dev,
                                            device_id_type=MESH)

    barrier = pltpu.get_barrier_semaphore()
    pl.semaphore_signal(barrier, inc=1, device_id={"freq": other}, device_id_type=MESH)
    for p in plane:
        pl.semaphore_signal(barrier, inc=1, device_id={"row": p}, device_id_type=MESH)

    @pl.when(z > 0)
    def _():
        pl.semaphore_signal(barrier, inc=1, device_id={"col": z - 1}, device_id_type=MESH)

    @pl.when(z < cols_n - 1)
    def _():
        pl.semaphore_signal(barrier, inc=1, device_id={"col": z + 1}, device_id_type=MESH)

    mine = X.at[0, r]
    own = pltpu.make_async_copy(c_ref, mine, load.at[0])
    own.start()
    wown = pltpu.make_async_copy(w_ref, W.at[r], load.at[1])
    wown.start()
    acc[...] = jnp.zeros_like(acc)
    own.wait()
    wown.wait()
    pl.semaphore_wait(barrier, 1 + len(plane) + jnp.where(z > 0, 1, 0) + jnp.where(z < cols_n - 1, 1, 0))

    def w_copy(i):
        return rcopy(W.at[r], W.at[r], wsend.at[i], wrecv.at[i], {"row": plane[i]})

    def zsrc(q, k):
        return T.at[q, trow(k)]

    def z_own(k, up):
        src = X.at[0, r, rows_of(k, f)]
        return rcopy(src, T.at[z, trow(k)], (zup if up else zdn).at[z, k], zr.at[z, k],
                     {"col": z + 1 if up else z - 1})

    def z_fwd(q, k, up):
        return rcopy(zsrc(q, k), zsrc(q, k), (zup if up else zdn).at[q, k], zr.at[q, k],
                     {"col": z + 1 if up else z - 1})

    def n_own(k, to_x):
        src = X.at[0, r, rows_of(k, f)]
        return rcopy(src, src, (nx if to_x else ny).at[k], nr.at[0 if to_x else 1, k], {"row": xn if to_x else yn})

    def n_relay(k, from_x):
        src = X.at[0, xn if from_x else yn, rows_of(k, f)]
        return rcopy(src, src, nrl.at[k], nr.at[2, k], {"row": yn if from_x else xn})

    def m_copy(q, k):
        return rcopy(zsrc(q, k), X.at[1, r, rows_of(k, f)], ms.at[q, k], mr.at[r, k], {"row": q})

    def d_copy(m, b, k, core):
        src = X.at[m, b, rows_of(k, core)]
        return rcopy(src, src, ds.at[m, b, k], dr.at[m, b, k], {"freq": other})

    def d_start(m, b, k):
        d_copy(m, b, k, f).start()

    def own_first(k):
        return pltpu.make_async_copy(zsrc(r, k), X.at[1, r, rows_of(k, f)], tl.at[k])

    for i in range(3):
        w_copy(i).start()

    def start_own(k):
        @pl.when(z < cols_n - 1)
        def _():
            z_own(k, True).start()

        @pl.when(z > 0)
        def _():
            z_own(k, False).start()

        n_own(k, True).start()
        n_own(k, False).start()

    def z_arrive(q, k, go_up):
        z_fwd(q, k, go_up).wait_recv()
        if go_up:
            @pl.when(z < cols_n - 1)
            def _():
                z_fwd(q, k, True).start()
        else:
            @pl.when(z > 0)
            def _():
                z_fwd(q, k, False).start()

        @pl.when(q == r)
        def _():
            own_first(k).start()
            own_first(k).wait()
            d_start(1, r, k)

        @pl.when(q != r)
        def _():
            m_copy(q, k).start()

    def multiply(k):
        for b in range(rows_n):
            rows = pl.ds(pl.multiple_of(k * CH, CH), CH)
            first = X[mi, b, rows, :].astype(jnp.float32).T
            weighted = (first * W[b, pl.ds(k, 1), :]).astype(jnp.bfloat16)
            tile = width // 3
            for t in range(3):
                part = pl.ds(t * tile, tile)
                acc[:, part] += jnp.dot(weighted, X[0, b, rows, part], preferred_element_type=jnp.float32)

    start_own(0)
    for i in range(3):
        w_copy(i).wait_recv()

    SKEW = cols_n

    @pl.loop(0, K + SKEW)
    def _(k):
        @pl.when(k + 1 < K)
        def _():
            start_own(k + 1)

        for d in range(1, cols_n):
            kk = k - (d - 1)
            valid = (kk >= 0) & (kk < K)

            @pl.when(valid & (z - d >= 0))
            def _():
                z_arrive(z - d, kk, True)

            @pl.when(valid & (z + d < cols_n))
            def _():
                z_arrive(z + d, kk, False)

        @pl.when(k < K)
        def _():
            n_own(k, True).wait_recv()
            even = lax.rem(k, 2) == 0

            @pl.when(even)
            def _():
                n_relay(k, True).start()

            d_start(0, xn, k)
            n_own(k, False).wait_recv()

            @pl.when(jnp.logical_not(even))
            def _():
                n_relay(k, False).start()

            d_start(0, yn, k)

        @pl.when((k >= 1) & (k - 1 < K))
        def _():
            n_relay(k - 1, True).wait_recv()
            d_start(0, dg, k - 1)

        kl = k - SKEW + 1

        @pl.when((kl >= 0) & (kl < K) & (r != z))
        def _():
            for p in plane:
                rcopy(zsrc(r, kl), X.at[1, p, rows_of(kl, f)], ms.at[r, kl], mr.at[p, kl], {"row": p}).wait_recv()
                d_start(1, p, kl)

        km = k - SKEW

        @pl.when(km >= 0)
        def _():
            for p in plane:
                d_copy(0, p, km, other).wait_recv()

            @pl.when(r != z)
            def _():
                for b in range(rows_n):
                    d_copy(1, b, km, other).wait_recv()

            multiply(km)

    out = pltpu.make_async_copy(acc, o_ref, osem)
    out.start()

    for i in range(3):
        w_copy(i).wait_send()

    @pl.loop(0, K)
    def _(k):
        n_own(k, True).wait_send()
        n_own(k, False).wait_send()
        n_relay(k, True).wait_send()
        for p in plane:
            d_copy(0, p, k, f).wait_send()

        @pl.when(r != z)
        def _():
            for b in range(rows_n):
                d_copy(1, b, k, f).wait_send()

        for q in range(cols_n):
            @pl.when((q <= z) & (z < cols_n - 1))
            def _():
                z_fwd(q, k, True).wait_send()

            @pl.when((q >= z) & (z > 0))
            def _():
                z_fwd(q, k, False).wait_send()

            @pl.when((q != z) & (q != r))
            def _():
                m_copy(q, k).wait_send()

    out.wait()


def gathered_tile(cols_n, coupling, freq_weight):
    depth, width = coupling.shape
    CH = depth // 6
    K = depth // CH
    rows_n = SIDE * SIDE
    dma = pltpu.SemaphoreType.DMA
    return pl.pallas_call(
        functools.partial(kernel, cols_n, K, CH),
        out_shape=jax.ShapeDtypeStruct((width, width), jnp.float32),
        in_specs=[pl.BlockSpec(memory_space=pl.ANY)] * 2,
        out_specs=pl.BlockSpec(memory_space=pl.ANY),
        scratch_shapes=[
            pltpu.VMEM((2, rows_n, depth, width), jnp.bfloat16),
            pltpu.VMEM((cols_n, depth // 2, width), jnp.bfloat16),
            pltpu.VMEM((rows_n, K, CH), jnp.float32),
            pltpu.VMEM((width, width), jnp.float32),
            dma((2,)), dma((3,)), dma((3,)),
            dma((cols_n, K)), dma((cols_n, K)), dma((cols_n, K)), dma((K,)),
            dma((3, K)), dma((K,)), dma((K,)), dma((K,)),
            dma((cols_n, K)), dma((rows_n, K)), dma((2, rows_n, K)), dma((2, rows_n, K)), dma,
        ],
        compiler_params=pltpu.CompilerParams(
            collective_id=0, has_side_effects=True, vmem_limit_bytes=67043328
        ),
    )(coupling, freq_weight.reshape(K, CH))


def on_device(coupling, freq_weight):
    weighted = (coupling.astype(jnp.float32) * freq_weight[:, None]).astype(jnp.bfloat16)
    full_rows = lax.all_gather(weighted, "col", axis=1, tiled=True)
    return lax.psum_scatter(
        lax.dot_general(
            full_rows, coupling, (((0,), (0,)), ((), ())), preferred_element_type=jnp.float32
        ),
        "row",
        scatter_dimension=0,
        tiled=True,
    )


def solution(mesh):
    placed = (P("row", "col"), P(("freq", "row")))
    square = mesh.shape["freq"] == 2 and mesh.shape["row"] == SIDE * SIDE and mesh.shape["col"] == mesh.shape["row"]

    def step(coupling, freq_weight):
        depth, width = coupling.shape
        if square and depth == width and depth % (6 * 256) == 0:
            return gathered_tile(mesh.shape["col"], coupling, freq_weight)
        return on_device(coupling, freq_weight)

    return jax.shard_map(
        step, mesh=mesh, in_specs=placed, out_specs=P(("freq", "row"), "col"), check_vma=False
    )
```

```python
import functools

import jax
import jax.numpy as jnp
from jax import lax
from jax.experimental import pallas as pl
from jax.experimental.pallas import tpu as pltpu
from jax.sharding import PartitionSpec as P

MESH = pl.DeviceIdType.MESH
SIDE = 2


def kernel(cols_n, K, CH, c_ref, w_ref, o_ref, X, T, W, acc, load, wsend, wrecv, zr, zup, zdn, tl, nr, nx, ny, nrl,
           ms, mr, ds, dr, bup, bdn, br, osem):
    f = lax.axis_index("freq")
    r = lax.axis_index("row")
    z = lax.axis_index("col")
    rows_n = SIDE * SIDE
    H = CH // 2
    other = 1 - f
    xn, yn, dg = r ^ 1, r ^ 2, r ^ 3
    plane = (xn, yn, dg)
    mi = jnp.where(r == z, 0, 1)
    width = c_ref.shape[1]

    def rows_of(k, core):
        return pl.ds(pl.multiple_of(k * CH + core * H, H), H)

    def trow(k):
        return pl.ds(pl.multiple_of(k * H, H), H)

    def rcopy(src, dst, s, d, dev):
        return pltpu.make_async_remote_copy(src_ref=src, dst_ref=dst, send_sem=s, recv_sem=d, device_id=dev,
                                            device_id_type=MESH)

    barrier = pltpu.get_barrier_semaphore()
    pl.semaphore_signal(barrier, inc=1, device_id={"freq": other}, device_id_type=MESH)
    for p in plane:
        pl.semaphore_signal(barrier, inc=1, device_id={"row": p}, device_id_type=MESH)

    @pl.when(z > 0)
    def _():
        pl.semaphore_signal(barrier, inc=1, device_id={"col": z - 1}, device_id_type=MESH)

    @pl.when(z < cols_n - 1)
    def _():
        pl.semaphore_signal(barrier, inc=1, device_id={"col": z + 1}, device_id_type=MESH)

    mine = X.at[0, r]
    own = pltpu.make_async_copy(c_ref, mine, load.at[0])
    own.start()
    wown = pltpu.make_async_copy(w_ref, W.at[r], load.at[1])
    wown.start()
    own.wait()
    wown.wait()
    pl.semaphore_wait(barrier, 1 + len(plane) + jnp.where(z > 0, 1, 0) + jnp.where(z < cols_n - 1, 1, 0))

    def w_copy(i):
        return rcopy(W.at[r], W.at[r], wsend.at[i], wrecv.at[i], {"row": plane[i]})

    def zsrc(q, k):
        return T.at[q, trow(k)]

    def z_own(k, up):
        src = X.at[0, r, rows_of(k, f)]
        return rcopy(src, T.at[z, trow(k)], (zup if up else zdn).at[z, k], zr.at[z, k],
                     {"col": z + 1 if up else z - 1})

    def z_fwd(q, k, up):
        return rcopy(zsrc(q, k), zsrc(q, k), (zup if up else zdn).at[q, k], zr.at[q, k],
                     {"col": z + 1 if up else z - 1})

    def n_own(k, to_x):
        src = X.at[0, r, rows_of(k, f)]
        return rcopy(src, src, (nx if to_x else ny).at[k], nr.at[0 if to_x else 1, k], {"row": xn if to_x else yn})

    def n_relay(k, from_x):
        src = X.at[0, xn if from_x else yn, rows_of(k, f)]
        return rcopy(src, src, nrl.at[k], nr.at[2, k], {"row": yn if from_x else xn})

    def m_copy(q, k):
        return rcopy(zsrc(q, k), X.at[1, r, rows_of(k, f)], ms.at[q, k], mr.at[r, k], {"row": q})

    def d_copy(m, b, k, core):
        src = X.at[m, b, rows_of(k, core)]
        return rcopy(src, src, ds.at[m, b, k], dr.at[m, b, k], {"freq": other})

    def d_start(m, b, k):
        d_copy(m, b, k, f).start()

    def own_first(k):
        return pltpu.make_async_copy(zsrc(r, k), X.at[1, r, rows_of(k, f)], tl.at[k])

    for i in range(3):
        w_copy(i).start()

    def b_copy(b, up):
        return rcopy(X.at[mi, b, rows_of(0, f)], X.at[1, b, rows_of(0, f)], (bup if up else bdn).at[b], br.at[b],
                     {"col": z + 1 if up else z - 1})

    go_up, go_down = (z >= r) & (z < cols_n - 1), (z <= r) & (z > 0)
    dist = jnp.where(z > r, z - r, r - z)

    def b_send(b):
        @pl.when(go_up)
        def _():
            b_copy(b, True).start()

        @pl.when(go_down)
        def _():
            b_copy(b, False).start()

    def b_arrive(b):
        b_copy(b, True).wait_recv()
        b_send(b)
        d_start(1, b, 0)

    def start_own(k):
        @pl.when((z < cols_n - 1) & (k > 0))
        def _():
            z_own(k, True).start()

        @pl.when((z > 0) & (k > 0))
        def _():
            z_own(k, False).start()

        n_own(k, True).start()
        n_own(k, False).start()

    def z_arrive(q, k, go_up):
        z_fwd(q, k, go_up).wait_recv()
        if go_up:
            @pl.when(z < cols_n - 1)
            def _():
                z_fwd(q, k, True).start()
        else:
            @pl.when(z > 0)
            def _():
                z_fwd(q, k, False).start()

        @pl.when(q == r)
        def _():
            own_first(k).start()
            own_first(k).wait()
            d_start(1, r, k)

        @pl.when(q != r)
        def _():
            m_copy(q, k).start()

    def multiply(k):
        rows = pl.ds(pl.multiple_of(k * CH, CH), CH)
        for t in range(3):
            part = pl.ds(t * tile, tile)
            for b in range(rows_n):
                first = X[mi, b, rows, part].astype(jnp.float32).T
                weighted = (first * W[b, pl.ds(k, 1), :]).astype(jnp.bfloat16)
                acc[part, :] += jnp.dot(weighted, X[0, b, rows, :], preferred_element_type=jnp.float32)

            @pl.when(k == K - 1)
            def _():
                out_copy(t).start()

    tile = width // 3

    def out_copy(t):
        part = pl.ds(t * tile, tile)
        return pltpu.make_async_copy(acc.at[part], o_ref.at[part], osem.at[t])

    start_own(0)

    @pl.when(r == z)
    def _():
        b_send(r)

    acc[...] = jnp.zeros_like(acc)
    for i in range(3):
        w_copy(i).wait_recv()

    SKEW = cols_n

    @pl.loop(0, K + SKEW)
    def _(k):
        @pl.when(k + 1 < K)
        def _():
            start_own(k + 1)

        for d in range(1, cols_n):
            kk = k - (d - 1)
            valid = (kk >= 1) & (kk < K)

            @pl.when(valid & (z - d >= 0))
            def _():
                z_arrive(z - d, kk, True)

            @pl.when(valid & (z + d < cols_n))
            def _():
                z_arrive(z + d, kk, False)

        @pl.when(k < K)
        def _():
            n_own(k, True).wait_recv()
            even = lax.rem(k, 2) == 0

            @pl.when(even)
            def _():
                n_relay(k, True).start()

            d_start(0, xn, k)

            @pl.when((k == 0) & (r == z))
            def _():
                b_send(xn)

            n_own(k, False).wait_recv()

            @pl.when(jnp.logical_not(even))
            def _():
                n_relay(k, False).start()

            d_start(0, yn, k)

            @pl.when((k == 0) & (r == z))
            def _():
                b_send(yn)


        @pl.when((k >= 1) & (k - 1 < K))
        def _():
            n_relay(k - 1, True).wait_recv()
            d_start(0, dg, k - 1)

            @pl.when((k == 1) & (r == z))
            def _():
                b_send(dg)

        @pl.when((r != z) & (k == dist))
        def _():
            for b in (r, xn, yn):
                b_arrive(b)

        @pl.when((r != z) & (k == dist + 1))
        def _():
            b_arrive(dg)

        kl = k - SKEW + 1

        @pl.when((kl >= 1) & (kl < K) & (r != z))
        def _():
            for p in plane:
                rcopy(zsrc(r, kl), X.at[1, p, rows_of(kl, f)], ms.at[r, kl], mr.at[p, kl], {"row": p}).wait_recv()
                d_start(1, p, kl)

        km = k - SKEW

        @pl.when(km >= 0)
        def _():
            for p in plane:
                d_copy(0, p, km, other).wait_recv()

            @pl.when(r != z)
            def _():
                for b in range(rows_n):
                    d_copy(1, b, km, other).wait_recv()

            multiply(km)

    for i in range(3):
        w_copy(i).wait_send()
    for b in range(rows_n):
        @pl.when(go_up)
        def _():
            b_copy(b, True).wait_send()

        @pl.when(go_down)
        def _():
            b_copy(b, False).wait_send()

    @pl.loop(0, K)
    def _(k):
        n_own(k, True).wait_send()
        n_own(k, False).wait_send()
        n_relay(k, True).wait_send()
        for p in plane:
            d_copy(0, p, k, f).wait_send()

        @pl.when(r != z)
        def _():
            for b in range(rows_n):
                d_copy(1, b, k, f).wait_send()

        for q in range(cols_n):
            @pl.when((k > 0) & (q <= z) & (z < cols_n - 1))
            def _():
                z_fwd(q, k, True).wait_send()

            @pl.when((k > 0) & (q >= z) & (z > 0))
            def _():
                z_fwd(q, k, False).wait_send()

            @pl.when((k > 0) & (q != z) & (q != r))
            def _():
                m_copy(q, k).wait_send()

    for t in range(3):
        out_copy(t).wait()


def gathered_tile(cols_n, coupling, freq_weight):
    depth, width = coupling.shape
    CH = depth // 6
    K = depth // CH
    rows_n = SIDE * SIDE
    dma = pltpu.SemaphoreType.DMA
    return pl.pallas_call(
        functools.partial(kernel, cols_n, K, CH),
        out_shape=jax.ShapeDtypeStruct((width, width), jnp.float32),
        in_specs=[pl.BlockSpec(memory_space=pl.ANY)] * 2,
        out_specs=pl.BlockSpec(memory_space=pl.ANY),
        scratch_shapes=[
            pltpu.VMEM((2, rows_n, depth, width), jnp.bfloat16),
            pltpu.VMEM((cols_n, depth // 2, width), jnp.bfloat16),
            pltpu.VMEM((rows_n, K, CH), jnp.float32),
            pltpu.VMEM((width, width), jnp.float32),
            dma((2,)), dma((3,)), dma((3,)),
            dma((cols_n, K)), dma((cols_n, K)), dma((cols_n, K)), dma((K,)),
            dma((3, K)), dma((K,)), dma((K,)), dma((K,)),
            dma((cols_n, K)), dma((rows_n, K)), dma((2, rows_n, K)), dma((2, rows_n, K)),
            dma((rows_n,)), dma((rows_n,)), dma((rows_n,)), dma((3,)),
        ],
        compiler_params=pltpu.CompilerParams(
            collective_id=0, has_side_effects=True, vmem_limit_bytes=67043328
        ),
    )(coupling, freq_weight.reshape(K, CH))


def on_device(coupling, freq_weight):
    weighted = (coupling.astype(jnp.float32) * freq_weight[:, None]).astype(jnp.bfloat16)
    full_rows = lax.all_gather(weighted, "col", axis=1, tiled=True)
    return lax.psum_scatter(
        lax.dot_general(
            full_rows, coupling, (((0,), (0,)), ((), ())), preferred_element_type=jnp.float32
        ),
        "row",
        scatter_dimension=0,
        tiled=True,
    )


def solution(mesh):
    placed = (P("row", "col"), P(("freq", "row")))
    square = mesh.shape["freq"] == 2 and mesh.shape["row"] == SIDE * SIDE and mesh.shape["col"] == mesh.shape["row"]

    def step(coupling, freq_weight):
        depth, width = coupling.shape
        if square and depth == width and depth % (6 * 256) == 0:
            return gathered_tile(mesh.shape["col"], coupling, freq_weight)
        return on_device(coupling, freq_weight)

    return jax.shard_map(
        step, mesh=mesh, in_specs=placed, out_specs=P(("freq", "row"), "col"), check_vma=False
    )
```
